32 devices in a mesh: dp: 4 (over x, core), pipe: 2 (over y), tensor: 4 (over z).
Axes of the slice: x: 2, y: 2, z: 4, core: 2. Of those that a mesh axis runs over, the one named last changes fastest.
Arguments:
- weights: bfloat16 [2816, 1408], P(('dp', 'pipe', 'tensor')), may hold values from -6 to 6
- first_moment: bfloat16 [2816, 1408], P(('dp', 'pipe', 'tensor')), may hold values from -6 to 6
- second_moment: bfloat16 [2816, 1408], P(('dp', 'pipe', 'tensor')), may hold values from 0.049804688 to 5
- row_weight: float32 [1408], replicated, may hold values from -1 to 1
- col_weight: float32 [1408], replicated, may hold values from 1 to 4
Outputs:
- weight_tiles: bfloat16 [2816, 1408], P(('pipe', 'tensor'))
- first_tiles: bfloat16 [2816, 1408], P(('pipe', 'tensor'))
- second_tiles: bfloat16 [2816, 1408], P(('pipe', 'tensor'))
- checksums: float32 [3, 2, 4, 11], P(None, 'pipe', 'tensor')
The draws below stay inside these ranges and needn't reach their ends.
All inputs are finite; a program needn't handle non-finite values.
Results may differ from the reference program's by a relative error of at most 0.001.
Values may be sent and summed in bfloat16 or wider, within the bound.
A program may use at most 64 MiB of HBM per device.

```python
import math
import jax
import jax.numpy as jnp
from jax import lax

D = 1408
CHECK_COLS = 128
BLOCKS = 2
N_TENSOR = 4


def block_scale(key, dims, shards, low, high):
    gain = 1.0
    for position, blocks in shards:
        heights = jax.random.uniform(jax.random.fold_in(jax.random.fold_in(key, 6), position), (blocks,), jnp.float32, low / len(shards), high / len(shards))
        gain = gain * jnp.repeat(jnp.exp(heights), dims[position] // blocks).reshape((-1,) + (1,) * (len(dims) - 1 - position))
    return gain


def scatter_about(stream_key, dims, width, bound, pieces=(), kind=jnp.bfloat16):
    values = width * jax.random.normal(stream_key, dims, jnp.float32)
    if pieces:
        values = values * block_scale(stream_key, dims, pieces, -0.22, 0.18)
    return jnp.clip(values, -bound, bound).astype(kind)


def setup_inputs(seed: int = 0) -> dict:
    seeds = jax.random.split(jax.random.key(seed), 6)
    return {
        "weights": scatter_about(seeds[0], (BLOCKS * D, D), 1.0, 6.0, ((0, 32),)),
        "first_moment": scatter_about(seeds[1], (BLOCKS * D, D), 1.0, 6.0, ((0, 32),)),
        "second_moment": jnp.clip(jnp.exp(math.log(5.0) - 4.609084 * jax.random.uniform(seeds[2], (BLOCKS * D, D), jnp.float32) ** block_scale(seeds[2], (BLOCKS * D, D), ((0, 32),), -0.2, 0.2)), 0.049804688, 5.0).astype(jnp.bfloat16),
        "row_weight": jnp.clip(jax.random.uniform(seeds[3], (D,), jnp.float32, -1.0, 1.0), -1.0, 1.0),
        "col_weight": jnp.clip(jnp.exp(jax.random.uniform(seeds[4], (D,), jnp.float32, math.log(1.0), math.log(4.0))), 1.0, 4.0),
    }


def reference(weights, first_moment, second_moment, row_weight, col_weight):
    tile_rows = D // N_TENSOR
    col_blocks = D // CHECK_COLS
    factor = float(tile_rows * CHECK_COLS) ** -0.5
    row_grid = row_weight.reshape(N_TENSOR, tile_rows)
    col_grid = col_weight.reshape(col_blocks, CHECK_COLS)

    def one_kind(data):
        blocked = data.astype(jnp.float32).reshape(BLOCKS, N_TENSOR, tile_rows, col_blocks, CHECK_COLS)
        weighted = jnp.einsum("bjrce,jr->bjce", blocked, row_grid, precision=lax.Precision.HIGHEST)
        return factor * jnp.sum(weighted * col_grid, axis=3)

    checks = jnp.stack([one_kind(weights), one_kind(first_moment), one_kind(second_moment)]).astype(jnp.float32)
    return weights, first_moment, second_moment, checks
```

```python
import functools

import jax
import jax.numpy as jnp
from jax import lax
from jax.experimental import pallas as pl
from jax.experimental.pallas import tpu as pltpu
from jax.sharding import PartitionSpec as P

CHECK_COLS = 128


def for_sending(array):
    return jax.tree.map(lambda a: a.astype(jnp.bfloat16) if a.dtype == jnp.float32 else a, array)


def column_sums(data, row_part, col_weight, col_blocks):
    row_mixed = jnp.dot(
        row_part[None, :], data.astype(jnp.float32), precision=lax.Precision.HIGHEST
    )[0]
    return jnp.sum((row_mixed * col_weight).reshape(col_blocks, -1), axis=1)


def shards(weights, first_moment, second_moment, row_weight, col_weight):
    dp_count = lax.axis_size("dp")
    pipe_count = lax.axis_size("pipe")
    tensor_count = lax.axis_size("tensor")
    shard_rows, width = weights.shape
    dp_section = dp_count // pipe_count
    tile_shards = dp_count // tensor_count
    piece_cols = width // dp_count
    tile_rows = shard_rows * dp_count
    col_blocks = width // CHECK_COLS
    factor = float(tile_rows * CHECK_COLS) ** (-0.5)
    sources = (weights, first_moment, second_moment)
    exchanged = (
        lax.all_to_all(sources[0], "dp", split_axis=1, concat_axis=0, tiled=True),
        lax.all_to_all(sources[1], "dp", split_axis=1, concat_axis=0, tiled=True),
        lax.all_to_all(sources[2], "dp", split_axis=1, concat_axis=0, tiled=True),
    )
    grouped = tuple(
        (item.reshape(pipe_count, dp_section, shard_rows, piece_cols) for item in exchanged)
    )
    sectioned = jax.tree.map(
        lambda part, own: part.astype(own.dtype),
        lax.all_to_all(for_sending(grouped), "pipe", split_axis=0, concat_axis=2, tiled=True),
        grouped,
    )
    routed = tuple(
        (item.reshape(tensor_count, tile_shards, 1, shard_rows, piece_cols) for item in sectioned)
    )
    arrived = jax.tree.map(
        lambda part, own: part.astype(own.dtype),
        lax.all_to_all(for_sending(routed), "tensor", split_axis=0, concat_axis=2, tiled=True),
        routed,
    )
    flat_pieces = tuple((item.reshape(tile_rows, piece_cols) for item in arrived))
    tiles = jax.tree.map(
        lambda part, own: part.astype(own.dtype),
        lax.all_gather(for_sending(flat_pieces), "dp", axis=1, tiled=True),
        flat_pieces,
    )
    tensor_pos = lax.axis_index("tensor")
    flat_index = (
        lax.axis_index("dp") * pipe_count + lax.axis_index("pipe")
    ) * tensor_count + tensor_pos
    in_section = flat_index % (dp_count * tensor_count)
    section_of = flat_index // (dp_count * tensor_count)
    tile_of = in_section // dp_count
    row_part = lax.dynamic_slice_in_dim(row_weight, in_section * shard_rows, shard_rows)
    partial_value = jnp.stack(
        [column_sums(item, row_part, col_weight, col_blocks) for item in sources]
    )
    section_hit = (jnp.arange(pipe_count) == section_of).astype(jnp.float32)
    tile_hit = (jnp.arange(tensor_count) == tile_of).astype(jnp.float32)
    spread = (
        partial_value[:, None, None, :]
        * section_hit[None, :, None, None]
        * tile_hit[None, None, :, None]
    )
    summed = lax.psum(spread, ("dp", "pipe", "tensor"))
    checks = (
        lax.dynamic_slice(summed, (0, lax.axis_index("pipe"), tensor_pos, 0), (3, 1, 1, col_blocks))
        * factor
    )
    return (tiles[0], tiles[1], tiles[2], checks)


def remote(src, dst, send_sem, recv_sem, where):
    return pltpu.make_async_remote_copy(
        src_ref=src,
        dst_ref=dst,
        send_sem=send_sem,
        recv_sem=recv_sem,
        device_id=where,
        device_id_type=pl.DeviceIdType.MESH,
    )


def route(
    count,
    w_ref,
    m_ref,
    v_ref,
    row_ref,
    col_ref,
    out0,
    out1,
    out2,
    check_ref,
    src,
    crossed,
    own,
    transit,
    acc,
    row_terms,
    load_sem,
    cross_send,
    cross_recv,
    z_send,
    own_recv,
    transit_recv,
    x_send,
    y_send,
    d_send,
    out_sem,
):
    dp, y, z = lax.axis_index("dp"), lax.axis_index("pipe"), lax.axis_index("tensor")
    x, core = dp // 2, dp % 2
    active = z // 2 == core
    diag = x == y
    to_x = {"dp": (1 - x) * 2 + core, "pipe": y, "tensor": z}
    to_y = {"dp": dp, "pipe": 1 - y, "tensor": z}
    to_core = {"dp": x * 2 + 1 - core, "pipe": y, "tensor": z}

    def to_z(pos):
        return {"dp": dp, "pipe": y, "tensor": pos}

    rows, width = w_ref.shape
    ins = (w_ref, m_ref, v_ref)
    outs = (out0, out1, out2)
    loads = [pltpu.make_async_copy(ins[a], src.at[a], load_sem.at[a]) for a in range(3)]
    for load in loads:
        load.start()

    barrier = pltpu.get_barrier_semaphore()
    for where in (to_x, to_y, to_core):
        pl.semaphore_signal(barrier, inc=1, device_id=where, device_id_type=pl.DeviceIdType.MESH)
    for step in range(1, count):
        pl.semaphore_signal(
            barrier,
            inc=1,
            device_id=to_z((z + step) % count),
            device_id_type=pl.DeviceIdType.MESH,
        )
    pl.semaphore_wait(barrier, count + 2)
    for load in loads:
        load.wait()

    cross_a = remote(src.at[2], crossed.at[0], cross_send.at[0], cross_recv.at[0], to_y)
    cross_b = [
        remote(src.at[a], crossed.at[a], cross_send.at[a], cross_recv.at[a], to_y) for a in range(2)
    ]

    def z_copies(pos, turn, pieces, act):
        for a, piece, slot, sem in pieces:
            away = remote(piece, slot, z_send.at[turn, a], sem, to_z(pos))
            near = pltpu.make_async_copy(piece, slot, sem)

            @pl.when(pos != z)
            def _():
                if act == "start":
                    away.start()
                else:
                    away.wait_send()

            if act == "start":

                @pl.when(pos == z)
                def _():
                    near.start()

    mine, other = 2 * core + y, 2 * core + 1 - y
    diag_mine = [(a, src.at[a], own.at[a, z], own_recv.at[a, z]) for a in range(2)]
    diag_other = [(a, crossed.at[a], own.at[a, z], own_recv.at[a, z]) for a in range(2)]
    off_mine = [(0, src.at[2], transit.at[z], transit_recv.at[z])]
    off_other = [(0, crossed.at[0], transit.at[z], transit_recv.at[z])]

    @pl.when(diag)
    def _():
        cross_a.start()
        z_copies(mine, 0, diag_mine, "start")

    @pl.when(jnp.logical_not(diag))
    def _():
        for copy in cross_b:
            copy.start()
        z_copies(mine, 0, off_mine, "start")

    for k in range(count):
        first = (z * count + k) * rows
        everyone = jnp.broadcast_to(row_ref[...].reshape(1, width), (8, width))
        part = pltpu.roll(everyone, (width - first) % width, 1)[:, :rows]
        high = part.astype(jnp.bfloat16).astype(jnp.float32)
        middle = (part - high).astype(jnp.bfloat16).astype(jnp.float32)
        low = part - high - middle
        line = lax.broadcasted_iota(jnp.int32, (8, rows), 0)
        terms = jnp.where(
            line == 0, high, jnp.where(line == 1, middle, jnp.where(line == 2, low, 0.0))
        )
        row_terms[k] = terms.astype(jnp.bfloat16)
    acc[...] = jnp.zeros_like(acc)

    @pl.when(diag)
    def _():
        for copy in cross_b:
            copy.wait_recv()
        z_copies(other, 1, diag_other, "start")

    @pl.when(jnp.logical_not(diag))
    def _():
        cross_a.wait_recv()
        z_copies(other, 1, off_other, "start")

    def arrived(a, k):
        pltpu.make_async_copy(own.at[a, k], own.at[a, k], own_recv.at[a, k]).wait()

    def passed(k):
        pltpu.make_async_copy(transit.at[k], transit.at[k], transit_recv.at[k]).wait()

    def own_x(a, k):
        return remote(own.at[a, k], own.at[a, k], x_send.at[a, k], own_recv.at[a, k], to_x)

    def transit_x(k):
        return remote(transit.at[k], transit.at[k], x_send.at[0, k], transit_recv.at[k], to_x)

    def transit_y(k):
        return remote(transit.at[k], own.at[2, k], y_send.at[k], own_recv.at[2, k], to_y)

    def across(a, k):
        return remote(own.at[a, k], own.at[a, k], d_send.at[a, k], own_recv.at[a, k], to_core)

    def leave(a, k):
        return pltpu.make_async_copy(own.at[a, k], outs[a].at[k], out_sem.at[a, k])

    @pl.loop(0, count)
    def _(step):
        k = jnp.where(z < count // 2, (z + step) % count, (z + count - step) % count)

        @pl.when(jnp.logical_and(active, diag))
        def _():
            for a in range(2):
                arrived(a, k)
                own_x(a, k).start()
                across(a, k).start()
            passed(k)
            transit_y(k).start()
            arrived(2, k)
            across(2, k).start()

        @pl.when(jnp.logical_and(active, jnp.logical_not(diag)))
        def _():
            passed(k)
            transit_y(k).start()
            transit_x(k).start()
            for a in range(3):
                arrived(a, k)
                across(a, k).start()

        @pl.when(jnp.logical_not(active))
        def _():
            for a in range(3):
                arrived(a, k)

        for a in range(3):
            leave(a, k).start()

        for a in range(3):
            acc[a] += jnp.dot(row_terms[k], own[a, k], preferred_element_type=jnp.float32)

    factor = float(rows * count * CHECK_COLS) ** (-0.5)
    blocks = width // CHECK_COLS
    weight = col_ref[...].reshape(1, width)
    for a in range(3):
        mixed = jnp.sum(acc[a], axis=0, keepdims=True) * weight
        lane = lax.broadcasted_iota(jnp.int32, (1, blocks), 1)
        line = jnp.zeros((1, blocks), jnp.float32)
        for e in range(blocks):
            part = jnp.sum(mixed[:, e * CHECK_COLS : (e + 1) * CHECK_COLS], axis=1, keepdims=True)
            line = jnp.where(lane == e, part, line)
        check_ref[a, 0] = line * factor

    @pl.when(diag)
    def _():
        cross_a.wait_send()
        z_copies(mine, 0, diag_mine, "wait")
        z_copies(other, 1, diag_other, "wait")

    @pl.when(jnp.logical_not(diag))
    def _():
        for copy in cross_b:
            copy.wait_send()
        z_copies(mine, 0, off_mine, "wait")
        z_copies(other, 1, off_other, "wait")

    @pl.loop(0, count)
    def _(k):
        @pl.when(active)
        def _():
            for a in range(3):
                across(a, k).wait_send()
            transit_y(k).wait_send()

            @pl.when(diag)
            def _():
                for a in range(2):
                    own_x(a, k).wait_send()

            @pl.when(jnp.logical_not(diag))
            def _():
                transit_x(k).wait_send()

        for a in range(3):
            leave(a, k).wait()


def routed(weights, first_moment, second_moment, row_weight, col_weight):
    count = lax.axis_size("dp")
    rows, width = weights.shape
    blocks = width // CHECK_COLS
    vmem = pl.BlockSpec(memory_space=pltpu.VMEM)
    anywhere = pl.BlockSpec(memory_space=pl.ANY)
    tile = jax.ShapeDtypeStruct((count, rows, width), weights.dtype)
    dma = pltpu.SemaphoreType.DMA
    out = pl.pallas_call(
        functools.partial(route, count),
        out_shape=(tile, tile, tile, jax.ShapeDtypeStruct((3, 1, 1, blocks), jnp.float32)),
        in_specs=[anywhere, anywhere, anywhere, vmem, vmem],
        out_specs=(anywhere, anywhere, anywhere, vmem),
        scratch_shapes=[
            pltpu.VMEM((3, rows, width), weights.dtype),
            pltpu.VMEM((2, rows, width), weights.dtype),
            pltpu.VMEM((3, count, rows, width), weights.dtype),
            pltpu.VMEM((count, rows, width), weights.dtype),
            pltpu.VMEM((3, 8, width), jnp.float32),
            pltpu.VMEM((count, 8, rows), jnp.bfloat16),
            dma((3,)),
            dma((2,)),
            dma((2,)),
            dma((2, 2)),
            dma((3, count)),
            dma((count,)),
            dma((2, count)),
            dma((count,)),
            dma((3, count)),
            dma((3, count)),
        ],
        compiler_params=pltpu.CompilerParams(collective_id=0, has_side_effects=True),
    )(weights, first_moment, second_moment, row_weight, col_weight)
    return tuple(item.reshape(count * rows, width) for item in out[:3]) + (out[3],)


def solution(mesh):
    dp_count, pipe_count, tensor_count = (mesh.shape[a] for a in ("dp", "pipe", "tensor"))
    square = dp_count == tensor_count == 2 * pipe_count and pipe_count == 2
    return jax.shard_map(
        routed if square else shards,
        mesh=mesh,
        in_specs=(
            P(("dp", "pipe", "tensor"), None),
            P(("dp", "pipe", "tensor"), None),
            P(("dp", "pipe", "tensor"), None),
            P(),
            P(),
        ),
        out_specs=(
            P(("pipe", "tensor"), None),
            P(("pipe", "tensor"), None),
            P(("pipe", "tensor"), None),
            P(None, "pipe", "tensor", None),
        ),
        check_vma=False,
    )
```

```python
import functools

import jax
import jax.numpy as jnp
from jax import lax
from jax.experimental import pallas as pl
from jax.experimental.pallas import tpu as pltpu
from jax.sharding import PartitionSpec as P

CHECK_COLS = 128


def for_sending(array):
    return jax.tree.map(lambda a: a.astype(jnp.bfloat16) if a.dtype == jnp.float32 else a, array)


def column_sums(data, row_part, col_weight, col_blocks):
    row_mixed = jnp.dot(
        row_part[None, :], data.astype(jnp.float32), precision=lax.Precision.HIGHEST
    )[0]
    return jnp.sum((row_mixed * col_weight).reshape(col_blocks, -1), axis=1)


def shards(weights, first_moment, second_moment, row_weight, col_weight):
    dp_count = lax.axis_size("dp")
    pipe_count = lax.axis_size("pipe")
    tensor_count = lax.axis_size("tensor")
    shard_rows, width = weights.shape
    dp_section = dp_count // pipe_count
    tile_shards = dp_count // tensor_count
    piece_cols = width // dp_count
    tile_rows = shard_rows * dp_count
    col_blocks = width // CHECK_COLS
    factor = float(tile_rows * CHECK_COLS) ** (-0.5)
    sources = (weights, first_moment, second_moment)
    exchanged = (
        lax.all_to_all(sources[0], "dp", split_axis=1, concat_axis=0, tiled=True),
        lax.all_to_all(sources[1], "dp", split_axis=1, concat_axis=0, tiled=True),
        lax.all_to_all(sources[2], "dp", split_axis=1, concat_axis=0, tiled=True),
    )
    grouped = tuple(
        (item.reshape(pipe_count, dp_section, shard_rows, piece_cols) for item in exchanged)
    )
    sectioned = jax.tree.map(
        lambda part, own: part.astype(own.dtype),
        lax.all_to_all(for_sending(grouped), "pipe", split_axis=0, concat_axis=2, tiled=True),
        grouped,
    )
    routed = tuple(
        (item.reshape(tensor_count, tile_shards, 1, shard_rows, piece_cols) for item in sectioned)
    )
    arrived = jax.tree.map(
        lambda part, own: part.astype(own.dtype),
        lax.all_to_all(for_sending(routed), "tensor", split_axis=0, concat_axis=2, tiled=True),
        routed,
    )
    flat_pieces = tuple((item.reshape(tile_rows, piece_cols) for item in arrived))
    tiles = jax.tree.map(
        lambda part, own: part.astype(own.dtype),
        lax.all_gather(for_sending(flat_pieces), "dp", axis=1, tiled=True),
        flat_pieces,
    )
    tensor_pos = lax.axis_index("tensor")
    flat_index = (
        lax.axis_index("dp") * pipe_count + lax.axis_index("pipe")
    ) * tensor_count + tensor_pos
    in_section = flat_index % (dp_count * tensor_count)
    section_of = flat_index // (dp_count * tensor_count)
    tile_of = in_section // dp_count
    row_part = lax.dynamic_slice_in_dim(row_weight, in_section * shard_rows, shard_rows)
    partial_value = jnp.stack(
        [column_sums(item, row_part, col_weight, col_blocks) for item in sources]
    )
    section_hit = (jnp.arange(pipe_count) == section_of).astype(jnp.float32)
    tile_hit = (jnp.arange(tensor_count) == tile_of).astype(jnp.float32)
    spread = (
        partial_value[:, None, None, :]
        * section_hit[None, :, None, None]
        * tile_hit[None, None, :, None]
    )
    summed = lax.psum(spread, ("dp", "pipe", "tensor"))
    checks = (
        lax.dynamic_slice(summed, (0, lax.axis_index("pipe"), tensor_pos, 0), (3, 1, 1, col_blocks))
        * factor
    )
    return (tiles[0], tiles[1], tiles[2], checks)


def remote(src, dst, send_sem, recv_sem, where):
    return pltpu.make_async_remote_copy(
        src_ref=src,
        dst_ref=dst,
        send_sem=send_sem,
        recv_sem=recv_sem,
        device_id=where,
        device_id_type=pl.DeviceIdType.MESH,
    )


def route(
    count,
    w_ref,
    m_ref,
    v_ref,
    own,
    src,
    crossed,
    transit,
    load_sem,
    cross_send,
    cross_recv,
    z_send,
    own_recv,
    transit_recv,
    x_send,
    y_send,
    d_send,
):
    dp, y, z = lax.axis_index("dp"), lax.axis_index("pipe"), lax.axis_index("tensor")
    x, core = dp // 2, dp % 2
    active = z // 2 == core
    diag = x == y
    to_x = {"dp": (1 - x) * 2 + core, "pipe": y, "tensor": z}
    to_y = {"dp": dp, "pipe": 1 - y, "tensor": z}
    to_core = {"dp": x * 2 + 1 - core, "pipe": y, "tensor": z}

    def to_z(pos):
        return {"dp": dp, "pipe": y, "tensor": pos}

    ins = (w_ref, m_ref, v_ref)
    loads = [pltpu.make_async_copy(ins[a], src.at[a], load_sem.at[a]) for a in range(3)]
    for load in loads:
        load.start()

    barrier = pltpu.get_barrier_semaphore()
    for where in (to_x, to_y, to_core):
        pl.semaphore_signal(barrier, inc=1, device_id=where, device_id_type=pl.DeviceIdType.MESH)
    for step in range(1, count):
        pl.semaphore_signal(
            barrier,
            inc=1,
            device_id=to_z((z + step) % count),
            device_id_type=pl.DeviceIdType.MESH,
        )
    pl.semaphore_wait(barrier, count + 2)
    for load in loads:
        load.wait()

    def cross(a):
        return remote(src.at[a], crossed, cross_send, cross_recv, to_y)

    def z_copies(pos, turn, pieces, act):
        for a, piece, slot, sem in pieces:
            away = remote(piece, slot, z_send.at[turn, a], sem, to_z(pos))
            near = pltpu.make_async_copy(piece, slot, sem)

            @pl.when(pos != z)
            def _():
                if act == "start":
                    away.start()
                else:
                    away.wait_send()

            if act == "start":

                @pl.when(pos == z)
                def _():
                    near.start()

    mine, other = 2 * core + y, 2 * core + 1 - y
    diag_mine = [(a, src.at[a], own.at[a, z], own_recv.at[a, z]) for a in (0, 1)]
    diag_other = [(0, crossed, own.at[0, z], own_recv.at[0, z])]
    off_mine = [(a - 1, src.at[a], transit.at[a - 1, z], transit_recv.at[a - 1, z]) for a in (1, 2)]
    off_other = [(0, crossed, transit.at[1, z], transit_recv.at[1, z])]

    @pl.when(diag)
    def _():
        cross(2).start()
        z_copies(mine, 0, diag_mine, "start")
        cross(2).wait_recv()
        z_copies(other, 1, diag_other, "start")

    @pl.when(jnp.logical_not(diag))
    def _():
        cross(0).start()
        z_copies(mine, 0, off_mine, "start")
        cross(0).wait_recv()
        z_copies(other, 1, off_other, "start")

    def arrived(a, k):
        pltpu.make_async_copy(own.at[a, k], own.at[a, k], own_recv.at[a, k]).wait()

    def passed(a, k):
        slot = transit.at[a - 1, k]
        pltpu.make_async_copy(slot, slot, transit_recv.at[a - 1, k]).wait()

    def own_x(a, k):
        return remote(own.at[a, k], own.at[a, k], x_send.at[a, k], own_recv.at[a, k], to_x)

    def transit_x(a, k):
        slot = transit.at[a - 1, k]
        return remote(slot, slot, x_send.at[a - 1, k], transit_recv.at[a - 1, k], to_x)

    def transit_y(a, k):
        return remote(
            transit.at[a - 1, k], own.at[a, k], y_send.at[a - 1, k], own_recv.at[a, k], to_y
        )

    def across(a, k):
        return remote(own.at[a, k], own.at[a, k], d_send.at[a, k], own_recv.at[a, k], to_core)

    half = count // 2

    def piece(step):
        if step < half:
            return jnp.where(
                z < half, (z + half - step) % half, half + (z - half + half - step) % half
            )
        return jnp.where(z < half, step, count - 1 - step)

    match = z % 2 == y

    def forward(on_diag, on_match):
        direct, passing, late = ((0, 1), (1, 2), (2,)) if on_match else ((0,), (2,), (1, 2))
        for step in range(count + 2):
            if step < count:
                k = piece(step)
                if on_diag:
                    for a in direct:
                        arrived(a, k)
                        own_x(a, k).start()
                        across(a, k).start()
                else:
                    for a in passing:
                        passed(a, k)
                        transit_x(a, k).start()
                        transit_y(a, k).start()
            if 1 <= step <= count:
                k = piece(step - 1)
                if on_diag:
                    for a in passing:
                        passed(a, k)
                        transit_y(a, k).start()
                else:
                    for a in direct:
                        arrived(a, k)
                        across(a, k).start()
            if step >= 2:
                k = piece(step - 2)
                for a in late:
                    arrived(a, k)
                    across(a, k).start()
        for k in range(count):
            for a in range(3):
                across(a, k).wait_send()
            for a in passing:
                transit_y(a, k).wait_send()
                if not on_diag:
                    transit_x(a, k).wait_send()
            if on_diag:
                for a in direct:
                    own_x(a, k).wait_send()

    for on_diag in (True, False):
        for on_match in (True, False):

            @pl.when(active & (diag == on_diag) & (match == on_match))
            def _():
                forward(on_diag, on_match)

    @pl.when(jnp.logical_not(active))
    def _():
        for k in range(count):
            for a in range(3):
                arrived(a, k)

    @pl.when(diag)
    def _():
        cross(2).wait_send()
        z_copies(mine, 0, diag_mine, "wait")
        z_copies(other, 1, diag_other, "wait")

    @pl.when(jnp.logical_not(diag))
    def _():
        cross(0).wait_send()
        z_copies(mine, 0, off_mine, "wait")
        z_copies(other, 1, off_other, "wait")


def finish(count, own, row_ref, col_ref, out0, out1, out2, check_ref, acc, out_sem):
    rows, width = own.shape[2:]
    outs = (out0, out1, out2)
    leaving = [pltpu.make_async_copy(own.at[a], outs[a], out_sem.at[a]) for a in range(3)]
    for copy in leaving:
        copy.start()
    acc[...] = jnp.zeros_like(acc)
    for k in range(count):
        first = (lax.axis_index("tensor") * count + k) * rows
        everyone = jnp.broadcast_to(row_ref[...].reshape(1, width), (8, width))
        part = pltpu.roll(everyone, (width - first) % width, 1)[:, :rows]
        high = part.astype(jnp.bfloat16).astype(jnp.float32)
        middle = (part - high).astype(jnp.bfloat16).astype(jnp.float32)
        low = part - high - middle
        line = lax.broadcasted_iota(jnp.int32, (8, rows), 0)
        terms = jnp.where(
            line == 0, high, jnp.where(line == 1, middle, jnp.where(line == 2, low, 0.0))
        )
        terms = terms.astype(jnp.bfloat16)
        for a in range(3):
            acc[a] += jnp.dot(terms, own[a, k], preferred_element_type=jnp.float32)

    factor = float(rows * count * CHECK_COLS) ** (-0.5)
    blocks = width // CHECK_COLS
    weight = col_ref[...].reshape(1, width)
    for a in range(3):
        mixed = jnp.sum(acc[a], axis=0, keepdims=True) * weight
        lane = lax.broadcasted_iota(jnp.int32, (1, blocks), 1)
        line = jnp.zeros((1, blocks), jnp.float32)
        for e in range(blocks):
            part = jnp.sum(mixed[:, e * CHECK_COLS : (e + 1) * CHECK_COLS], axis=1, keepdims=True)
            line = jnp.where(lane == e, part, line)
        check_ref[a, 0] = line * factor
    for copy in leaving:
        copy.wait()


def routed(weights, first_moment, second_moment, row_weight, col_weight):
    count = lax.axis_size("dp")
    rows, width = weights.shape
    blocks = width // CHECK_COLS
    vmem = pl.BlockSpec(memory_space=pltpu.VMEM)
    anywhere = pl.BlockSpec(memory_space=pl.ANY)
    tile = jax.ShapeDtypeStruct((count, rows, width), weights.dtype)
    dma = pltpu.SemaphoreType.DMA
    own = pl.pallas_call(
        functools.partial(route, count),
        out_shape=pltpu.VMEM((3, count, rows, width), weights.dtype),
        in_specs=[anywhere] * 3,
        out_specs=vmem,
        scratch_shapes=[
            pltpu.VMEM((3, rows, width), weights.dtype),
            pltpu.VMEM((rows, width), weights.dtype),
            pltpu.VMEM((2, count, rows, width), weights.dtype),
            dma((3,)),
            dma(()),
            dma(()),
            dma((2, 2)),
            dma((3, count)),
            dma((2, count)),
            dma((2, count)),
            dma((2, count)),
            dma((3, count)),
        ],
        compiler_params=pltpu.CompilerParams(
            collective_id=0, has_side_effects=True
        ),
    )(weights, first_moment, second_moment)
    out = pl.pallas_call(
        functools.partial(finish, count),
        out_shape=(tile, tile, tile, jax.ShapeDtypeStruct((3, 1, 1, blocks), jnp.float32)),
        in_specs=[vmem, vmem, vmem],
        out_specs=(anywhere, anywhere, anywhere, vmem),
        scratch_shapes=[pltpu.VMEM((3, 8, width), jnp.float32), dma((3,))],
        compiler_params=pltpu.CompilerParams(vmem_limit_bytes=16 * 1024 * 1024),
    )(own, row_weight, col_weight)
    return tuple(item.reshape(count * rows, width) for item in out[:3]) + (out[3],)


def solution(mesh):
    dp_count, pipe_count, tensor_count = (mesh.shape[a] for a in ("dp", "pipe", "tensor"))
    square = dp_count == tensor_count == 2 * pipe_count and pipe_count == 2
    return jax.shard_map(
        routed if square else shards,
        mesh=mesh,
        in_specs=(
            P(("dp", "pipe", "tensor"), None),
            P(("dp", "pipe", "tensor"), None),
            P(("dp", "pipe", "tensor"), None),
            P(),
            P(),
        ),
        out_specs=(
            P(("pipe", "tensor"), None),
            P(("pipe", "tensor"), None),
            P(("pipe", "tensor"), None),
            P(None, "pipe", "tensor", None),
        ),
        check_vma=False,
    )
```

```python
import functools

import jax
import jax.numpy as jnp
from jax import lax
from jax.experimental import pallas as pl
from jax.experimental.pallas import tpu as pltpu
from jax.sharding import PartitionSpec as P

CHECK_COLS = 128
SPLIT = 2
LEAD, START, HOP = 1.5, 2.5, 1.7


def for_sending(array):
    return jax.tree.map(lambda a: a.astype(jnp.bfloat16) if a.dtype == jnp.float32 else a, array)


def column_sums(data, row_part, col_weight, col_blocks):
    row_mixed = jnp.dot(
        row_part[None, :], data.astype(jnp.float32), precision=lax.Precision.HIGHEST
    )[0]
    return jnp.sum((row_mixed * col_weight).reshape(col_blocks, -1), axis=1)


def shards(weights, first_moment, second_moment, row_weight, col_weight):
    dp_count = lax.axis_size("dp")
    pipe_count = lax.axis_size("pipe")
    tensor_count = lax.axis_size("tensor")
    shard_rows, width = weights.shape
    dp_section = dp_count // pipe_count
    tile_shards = dp_count // tensor_count
    piece_cols = width // dp_count
    tile_rows = shard_rows * dp_count
    col_blocks = width // CHECK_COLS
    factor = float(tile_rows * CHECK_COLS) ** (-0.5)
    sources = (weights, first_moment, second_moment)
    exchanged = (
        lax.all_to_all(sources[0], "dp", split_axis=1, concat_axis=0, tiled=True),
        lax.all_to_all(sources[1], "dp", split_axis=1, concat_axis=0, tiled=True),
        lax.all_to_all(sources[2], "dp", split_axis=1, concat_axis=0, tiled=True),
    )
    grouped = tuple(
        (item.reshape(pipe_count, dp_section, shard_rows, piece_cols) for item in exchanged)
    )
    sectioned = jax.tree.map(
        lambda part, own: part.astype(own.dtype),
        lax.all_to_all(for_sending(grouped), "pipe", split_axis=0, concat_axis=2, tiled=True),
        grouped,
    )
    routed = tuple(
        (item.reshape(tensor_count, tile_shards, 1, shard_rows, piece_cols) for item in sectioned)
    )
    arrived = jax.tree.map(
        lambda part, own: part.astype(own.dtype),
        lax.all_to_all(for_sending(routed), "tensor", split_axis=0, concat_axis=2, tiled=True),
        routed,
    )
    flat_pieces = tuple((item.reshape(tile_rows, piece_cols) for item in arrived))
    tiles = jax.tree.map(
        lambda part, own: part.astype(own.dtype),
        lax.all_gather(for_sending(flat_pieces), "dp", axis=1, tiled=True),
        flat_pieces,
    )
    tensor_pos = lax.axis_index("tensor")
    flat_index = (
        lax.axis_index("dp") * pipe_count + lax.axis_index("pipe")
    ) * tensor_count + tensor_pos
    in_section = flat_index % (dp_count * tensor_count)
    section_of = flat_index // (dp_count * tensor_count)
    tile_of = in_section // dp_count
    row_part = lax.dynamic_slice_in_dim(row_weight, in_section * shard_rows, shard_rows)
    partial_value = jnp.stack(
        [column_sums(item, row_part, col_weight, col_blocks) for item in sources]
    )
    section_hit = (jnp.arange(pipe_count) == section_of).astype(jnp.float32)
    tile_hit = (jnp.arange(tensor_count) == tile_of).astype(jnp.float32)
    spread = (
        partial_value[:, None, None, :]
        * section_hit[None, :, None, None]
        * tile_hit[None, None, :, None]
    )
    summed = lax.psum(spread, ("dp", "pipe", "tensor"))
    checks = (
        lax.dynamic_slice(summed, (0, lax.axis_index("pipe"), tensor_pos, 0), (3, 1, 1, col_blocks))
        * factor
    )
    return (tiles[0], tiles[1], tiles[2], checks)


def remote(src, dst, send_sem, recv_sem, where):
    return pltpu.make_async_remote_copy(
        src_ref=src,
        dst_ref=dst,
        send_sem=send_sem,
        recv_sem=recv_sem,
        device_id=where,
        device_id_type=pl.DeviceIdType.MESH,
    )


def route(
    count,
    w_ref,
    m_ref,
    v_ref,
    own,
    src,
    crossed,
    transit,
    load_sem,
    cross_send,
    cross_recv,
    z_send,
    own_recv,
    transit_recv,
    x_send,
    y_send,
    d_send,
):
    dp, y, z = lax.axis_index("dp"), lax.axis_index("pipe"), lax.axis_index("tensor")
    x, core = dp // 2, dp % 2
    active = z // 2 == core
    diag = x == y
    to_x = {"dp": (1 - x) * 2 + core, "pipe": y, "tensor": z}
    to_y = {"dp": dp, "pipe": 1 - y, "tensor": z}
    to_core = {"dp": x * 2 + 1 - core, "pipe": y, "tensor": z}

    def to_z(pos):
        return {"dp": dp, "pipe": y, "tensor": pos}

    ins = (w_ref, m_ref, v_ref)
    loads = [pltpu.make_async_copy(ins[a], src.at[a], load_sem.at[a]) for a in range(3)]
    for load in loads:
        load.start()

    barrier = pltpu.get_barrier_semaphore()
    for where in (to_x, to_y, to_core):
        pl.semaphore_signal(barrier, inc=1, device_id=where, device_id_type=pl.DeviceIdType.MESH)
    for step in range(1, count):
        pl.semaphore_signal(
            barrier,
            inc=1,
            device_id=to_z((z + step) % count),
            device_id_type=pl.DeviceIdType.MESH,
        )
    pl.semaphore_wait(barrier, count + 2)
    for load in loads:
        load.wait()

    width = w_ref.shape[1]
    edges = [width // CHECK_COLS * h // SPLIT * CHECK_COLS for h in range(SPLIT)] + [width]
    cuts = [pl.ds(low, high - low) for low, high in zip(edges, edges[1:])]

    def own_at(a, k, h):
        return own.at[a, k, :, cuts[h]]

    def transit_at(a, k, h):
        return transit.at[a - 1, k, :, cuts[h]]

    def cross(a, h):
        return remote(
            src.at[a, :, cuts[h]],
            crossed.at[:, cuts[h]],
            cross_send.at[h],
            cross_recv.at[h],
            to_y,
        )

    def z_copies(pos, turn, pieces, act):
        for a, h, piece, slot, sem in pieces:
            away = remote(piece, slot, z_send.at[turn, a, h], sem, to_z(pos))
            near = pltpu.make_async_copy(piece, slot, sem)

            @pl.when(pos != z)
            def _():
                if act == "start":
                    away.start()
                else:
                    away.wait_send()

            if act == "start":

                @pl.when(pos == z)
                def _():
                    near.start()

    mine, other = 2 * core + y, 2 * core + 1 - y
    halves = range(len(cuts))

    def to_own(h, arrays, pieces):
        return [(n, h, p, own_at(a, z, h), own_recv.at[a, z, h]) for n, (a, p) in enumerate(zip(arrays, pieces))]

    def to_transit(h, arrays, pieces):
        return [
            (n, h, p, transit_at(a, z, h), transit_recv.at[a - 1, z, h])
            for n, (a, p) in enumerate(zip(arrays, pieces))
        ]

    def source(arrays, h):
        return [src.at[a, :, cuts[h]] for a in arrays]

    def mine_pieces(on_diag, h):
        if on_diag:
            return to_own(h, (0, 1), source((0, 1), h))
        return to_transit(h, (1, 2), source((1, 2), h))

    def other_pieces(on_diag, h):
        place, a = (to_own, 0) if on_diag else (to_transit, 2)
        return place(h, (a,), [crossed.at[:, cuts[h]]])

    for on_diag in (True, False):

        @pl.when(diag == on_diag)
        def _():
            sent = 2 if on_diag else 0
            for h in halves:
                cross(sent, h).start()
            for h in halves:
                z_copies(mine, 0, mine_pieces(on_diag, h), "start")
            for h in halves:
                cross(sent, h).wait_recv()
                z_copies(other, 1, other_pieces(on_diag, h), "start")

    def arrived(a, k, h):
        pltpu.make_async_copy(own_at(a, k, h), own_at(a, k, h), own_recv.at[a, k, h]).wait()

    def passed(a, k, h):
        slot = transit_at(a, k, h)
        pltpu.make_async_copy(slot, slot, transit_recv.at[a - 1, k, h]).wait()

    def own_x(a, k, h):
        slot = own_at(a, k, h)
        return remote(slot, slot, x_send.at[a, k, h], own_recv.at[a, k, h], to_x)

    def transit_x(a, k, h):
        slot = transit_at(a, k, h)
        return remote(slot, slot, x_send.at[a - 1, k, h], transit_recv.at[a - 1, k, h], to_x)

    def transit_y(a, k, h):
        return remote(
            transit_at(a, k, h),
            own_at(a, k, h),
            y_send.at[a - 1, k, h],
            own_recv.at[a, k, h],
            to_y,
        )

    def across(a, k, h):
        slot = own_at(a, k, h)
        return remote(slot, slot, d_send.at[a, k, h], own_recv.at[a, k, h], to_core)

    half = count // 2

    def piece(step):
        if step < half:
            return jnp.where(
                z < half, (z + half - step) % half, half + (z - half + half - step) % half
            )
        return jnp.where(z < half, step, count - 1 - step)

    match = z % 2 == y

    def in_turn(arrays, start, lag):
        turns = [(start + lag, a, 0) for a in arrays]
        for a in arrays:
            turns += [(start + lag + LEAD + len(turns) - len(arrays), a, s) for s in range(1, count)]
        return turns

    def forward(on_diag, on_match):
        direct, passing, late = ((0, 1), (1, 2), (2,)) if on_match else ((0,), (2,), (1, 2))
        start = 0.0 if on_match else START
        hop = HOP
        turns = [(t, "direct", a, s) for t, a, s in in_turn(direct, start, 0.0 if on_diag else hop)]
        turns += [(t, "pass", a, s) for t, a, s in in_turn(passing, start, hop if on_diag else 0.0)]
        turns += [(t, "late", a, s) for t, a, s in in_turn(late, START - start, 2 * hop + 0.1)]
        turns = [(t + 3 * h / SPLIT, way, a, step, h) for t, way, a, step in turns for h in halves]
        for _, way, a, step, h in sorted(turns):
            k = piece(step)
            if way == "pass":
                passed(a, k, h)
                transit_y(a, k, h).start()
                if not on_diag:
                    transit_x(a, k, h).start()
            else:
                arrived(a, k, h)
                if way == "direct" and on_diag:
                    own_x(a, k, h).start()
                across(a, k, h).start()

        @pl.loop(0, count)
        def _(k):
            for h in halves:
                for a in range(3):
                    across(a, k, h).wait_send()
                for a in passing:
                    transit_y(a, k, h).wait_send()
                    if not on_diag:
                        transit_x(a, k, h).wait_send()
                if on_diag:
                    for a in direct:
                        own_x(a, k, h).wait_send()

    for on_diag in (True, False):
        for on_match in (True, False):

            @pl.when(active & (diag == on_diag) & (match == on_match))
            def _():
                forward(on_diag, on_match)

    @pl.when(jnp.logical_not(active))
    def _():
        @pl.loop(0, count)
        def _(k):
            for a in range(3):
                for h in halves:
                    arrived(a, k, h)

    for on_diag in (True, False):

        @pl.when(diag == on_diag)
        def _():
            for h in halves:
                cross(2 if on_diag else 0, h).wait_send()
                z_copies(mine, 0, mine_pieces(on_diag, h), "wait")
                z_copies(other, 1, other_pieces(on_diag, h), "wait")


def finish(count, own, row_ref, col_ref, out0, out1, out2, check_ref, acc, out_sem):
    rows, width = own.shape[2:]
    outs = (out0, out1, out2)
    leaving = [pltpu.make_async_copy(own.at[a], outs[a], out_sem.at[a]) for a in range(3)]
    for copy in leaving:
        copy.start()
    acc[...] = jnp.zeros_like(acc)
    for k in range(count):
        first = (lax.axis_index("tensor") * count + k) * rows
        everyone = jnp.broadcast_to(row_ref[...].reshape(1, width), (8, width))
        part = pltpu.roll(everyone, (width - first) % width, 1)[:, :rows]
        high = part.astype(jnp.bfloat16).astype(jnp.float32)
        middle = (part - high).astype(jnp.bfloat16).astype(jnp.float32)
        low = part - high - middle
        line = lax.broadcasted_iota(jnp.int32, (8, rows), 0)
        terms = jnp.where(
            line == 0, high, jnp.where(line == 1, middle, jnp.where(line == 2, low, 0.0))
        )
        terms = terms.astype(jnp.bfloat16)
        for a in range(3):
            acc[a] += jnp.dot(terms, own[a, k], preferred_element_type=jnp.float32)

    factor = float(rows * count * CHECK_COLS) ** (-0.5)
    blocks = width // CHECK_COLS
    weight = col_ref[...].reshape(1, width)
    for a in range(3):
        mixed = jnp.sum(acc[a], axis=0, keepdims=True) * weight
        lane = lax.broadcasted_iota(jnp.int32, (1, blocks), 1)
        line = jnp.zeros((1, blocks), jnp.float32)
        for e in range(blocks):
            part = jnp.sum(mixed[:, e * CHECK_COLS : (e + 1) * CHECK_COLS], axis=1, keepdims=True)
            line = jnp.where(lane == e, part, line)
        check_ref[a, 0] = line * factor
    for copy in leaving:
        copy.wait()


def routed(weights, first_moment, second_moment, row_weight, col_weight):
    count = lax.axis_size("dp")
    rows, width = weights.shape
    blocks = width // CHECK_COLS
    vmem = pl.BlockSpec(memory_space=pltpu.VMEM)
    anywhere = pl.BlockSpec(memory_space=pl.ANY)
    tile = jax.ShapeDtypeStruct((count, rows, width), weights.dtype)
    dma = pltpu.SemaphoreType.DMA
    own = pl.pallas_call(
        functools.partial(route, count),
        out_shape=pltpu.VMEM((3, count, rows, width), weights.dtype),
        in_specs=[anywhere] * 3,
        out_specs=vmem,
        scratch_shapes=[
            pltpu.VMEM((3, rows, width), weights.dtype),
            pltpu.VMEM((rows, width), weights.dtype),
            pltpu.VMEM((2, count, rows, width), weights.dtype),
            dma((3,)),
            dma((SPLIT,)),
            dma((SPLIT,)),
            dma((2, 2, SPLIT)),
            dma((3, count, SPLIT)),
            dma((2, count, SPLIT)),
            dma((2, count, SPLIT)),
            dma((2, count, SPLIT)),
            dma((3, count, SPLIT)),
        ],
        compiler_params=pltpu.CompilerParams(
            collective_id=0, has_side_effects=True
        ),
    )(weights, first_moment, second_moment)
    out = pl.pallas_call(
        functools.partial(finish, count),
        out_shape=(tile, tile, tile, jax.ShapeDtypeStruct((3, 1, 1, blocks), jnp.float32)),
        in_specs=[vmem, vmem, vmem],
        out_specs=(anywhere, anywhere, anywhere, vmem),
        scratch_shapes=[pltpu.VMEM((3, 8, width), jnp.float32), dma((3,))],
        compiler_params=pltpu.CompilerParams(vmem_limit_bytes=16 * 1024 * 1024),
    )(own, row_weight, col_weight)
    return tuple(item.reshape(count * rows, width) for item in out[:3]) + (out[3],)


def solution(mesh):
    dp_count, pipe_count, tensor_count = (mesh.shape[a] for a in ("dp", "pipe", "tensor"))
    square = dp_count == tensor_count == 2 * pipe_count and pipe_count == 2
    return jax.shard_map(
        routed if square else shards,
        mesh=mesh,
        in_specs=(
            P(("dp", "pipe", "tensor"), None),
            P(("dp", "pipe", "tensor"), None),
            P(("dp", "pipe", "tensor"), None),
            P(),
            P(),
        ),
        out_specs=(
            P(("pipe", "tensor"), None),
            P(("pipe", "tensor"), None),
            P(("pipe", "tensor"), None),
            P(None, "pipe", "tensor", None),
        ),
        check_vma=False,
    )
```
